32 devices in a mesh: grp: 4 (over y, x), row: 8 (over z, core).
Axes of the slice: x: 2, y: 2, z: 4, core: 2. Of those that a mesh axis runs over, the one named last changes fastest.
Arguments:
- krylov_basis: bfloat16 [300, 512, 512], P(None, 'row', 'grp'), may hold values from -30 to 30
- krylov_image: bfloat16 [300, 512, 512], P(None, 'row', 'grp'), may hold values from -30 to 30
- tridiag_vectors: bfloat16 [300, 32], P(None, 'grp'), may hold values from -0.375 to 0.375
- ritz_values: bfloat16 [32], P('grp'), may hold values from -3 to 3
Outputs:
- ritz_vectors: float32 [32, 512, 512], P('grp', 'row')
- ritz_residuals: float32 [32, 512, 512], P('grp', 'row')
- residual_norms: float32 [32], P('grp')
The draws below stay inside these ranges and needn't reach their ends.
All inputs are finite; a program needn't handle non-finite values.
Results may differ from the reference program's by a relative error of at most 0.0003.
Values may be sent and summed in bfloat16 or wider, within the bound.
A program may use at most 64 MiB of HBM per device.

```python
import jax
import jax.numpy as jnp
from jax import lax

KRYLOV = 300
WANTED = 32
OUTER_DEV = 64
INNER_DEV = 128
OUTER = 512
INNER = 512
ROWS = 262144


def block_field(key):
    key_noise, key_scale, key_coef, key_common = jax.random.split(key, 4)
    blocks_outer = OUTER // OUTER_DEV
    blocks_inner = INNER // INNER_DEV
    noise_field = jax.random.normal(key_noise, (KRYLOV, OUTER, INNER), jnp.float32)
    levels = jax.random.uniform(key_scale, (blocks_outer, blocks_inner), jnp.float32, -0.7, 0.7)
    scales = jnp.exp(levels)
    scales = jnp.repeat(jnp.repeat(scales, OUTER_DEV, axis=0), INNER_DEV, axis=1)
    values_field = noise_field * scales[None, :, :]
    return jnp.clip(values_field, -30.0, 30.0).astype(jnp.bfloat16)


def draw_krylov_basis(key, part):
    return block_field(jax.random.fold_in(key, 11))


def draw_krylov_image(key, part):
    return block_field(jax.random.fold_in(key, 23))


def shard_levels(key, extent, pieces, least, high):
    factor_of, own = 1.0, jax.random.fold_in(key, 6)
    for dim, blocks in pieces:
        steps = jnp.exp(jax.random.uniform(jax.random.fold_in(own, dim), (blocks,), jnp.float32, least / len(pieces), high / len(pieces)))
        factor_of = factor_of * jnp.repeat(steps, extent[dim] // blocks).reshape([-1 if axis == dim else 1 for axis in range(len(extent))])
    return factor_of


def noise(rng, shape, width, bound, cuts=(), dtype=jnp.bfloat16):
    drawn = jax.random.normal(rng, shape, jnp.float32) * width
    if len(cuts) > 0:
        drawn = shard_levels(rng, shape, cuts, -0.22, 0.18) * drawn
    return jnp.clip(drawn, min=-bound, max=bound).astype(dtype)


def setup_inputs(seed: int = 0) -> dict:
    key_of = jax.random.split(jax.random.key(seed), 5)
    return {
        "krylov_basis": draw_krylov_basis(jax.random.fold_in(key_of[4], 71), 0),
        "krylov_image": draw_krylov_image(jax.random.fold_in(key_of[4], 71), 0),
        "tridiag_vectors": noise(key_of[2], (KRYLOV, WANTED), KRYLOV ** -0.5, 0.375, ((1, 4),)),
        "ritz_values": jnp.clip(jax.random.uniform(key_of[3], (WANTED,), jnp.float32, -3.0, 3.0) * shard_levels(key_of[3], (WANTED,), ((0, 4),), -0.4, 0.0), -3.0, 3.0).astype(jnp.bfloat16),
    }


def reference(krylov_basis, krylov_image, tridiag_vectors, ritz_values):
    flat_basis = krylov_basis.reshape(KRYLOV, OUTER * INNER)
    flat_image = krylov_image.reshape(KRYLOV, OUTER * INNER)
    coef_rows = tridiag_vectors.T
    ritz_cols = jnp.dot(coef_rows, flat_basis, preferred_element_type=jnp.float32)
    applied = jnp.dot(coef_rows, flat_image, preferred_element_type=jnp.float32)
    shift_values = ritz_values.astype(jnp.float32)
    resid_cols = applied - shift_values[:, None] * ritz_cols
    ritz_squares = lax.optimization_barrier(jnp.sum(ritz_cols * ritz_cols, axis=1)) + 1.0
    resid_squares = lax.optimization_barrier(jnp.sum(resid_cols * resid_cols, axis=1))
    factor = jnp.sqrt(ROWS / ritz_squares)
    ritz_vectors = (ritz_cols * factor[:, None]).reshape(WANTED, OUTER, INNER)
    ritz_residuals = (resid_cols * factor[:, None]).reshape(WANTED, OUTER, INNER)
    residual_norms = jnp.sqrt(resid_squares / ritz_squares)
    return (ritz_vectors, ritz_residuals, residual_norms)
```

```python
import functools
import math

import jax
import jax.numpy as jnp
from jax import lax
from jax.experimental import pallas as pl
from jax.experimental.pallas import tpu as pltpu
from jax.sharding import PartitionSpec as P

MESH = pl.DeviceIdType.MESH
TILE = 16
LANES = 128
SPREAD = 256.0
REACH = 86.0
SLOPE = 2.0 * REACH / math.log(1.0 + SPREAD)
LEAST = 1e-35


def cdiv(a, b):
    return (a + b - 1) // b


def grid_iota(shape, dim):
    return lax.broadcasted_iota(jnp.int32, shape, dim)


def expand_rows(cols, width):
    return jnp.broadcast_to(cols, (cols.shape[0], width)).reshape(cols.shape[0], 1, width)


def exchange_kernel(
    groups, rows, krylov_len,
    packed_ref, basis_ref, image_ref,
    coded_ref, stats_ref, total_ref,
    coefs, fields, spread, reps, expanded, coded, stat_send, stat_recv, row_send, row_recv,
    load_sem, coef_sems, data_sems, own_sem, stat_sems, row_sems,
):
    wanted_dev, packed_width = packed_ref.shape
    wanted = groups * wanted_dev
    chunks = fields.shape[1]
    inner_dev = basis_ref.shape[2]
    padded_len = fields.shape[2]
    steps = padded_len // TILE
    wide = TILE * TILE
    block = wanted_dev * TILE
    grp = lax.axis_index("grp")
    row = lax.axis_index("row")
    lane_stats = grid_iota((wanted, LANES), 1)

    def loads(chunk):
        span = pl.ds(pl.multiple_of(chunk * TILE, TILE), TILE)
        return [
            pltpu.make_async_copy(
                ref.at[:, span, :], fields.at[which, chunk, pl.ds(0, krylov_len)], load_sem.at[which, chunk]
            )
            for which, ref in enumerate((basis_ref, image_ref))
        ]

    for chunk in range(chunks):
        for copy in loads(chunk):
            copy.start()

    barrier = pltpu.get_barrier_semaphore()
    for step in range(1, groups):
        pl.semaphore_signal(barrier, inc=1, device_id={"grp": lax.rem(grp + step, groups)}, device_id_type=MESH)
    for step in range(1, rows):
        pl.semaphore_signal(barrier, inc=1, device_id={"row": lax.rem(row + step, rows)}, device_id_type=MESH)
    pl.semaphore_wait(barrier, groups + rows - 2)

    def remote(src, dst, sems, index, axis, step):
        me, size = (grp, groups) if axis == "grp" else (row, rows)
        return pltpu.make_async_remote_copy(
            src_ref=src,
            dst_ref=dst,
            send_sem=sems.at[(0,) + index],
            recv_sem=sems.at[(1,) + index],
            device_id={axis: lax.rem(me + step, size)},
            device_id_type=MESH,
        )

    def coef_copy(step):
        return remote(packed_ref, coefs.at[grp], coef_sems, (step,), "grp", step)

    for step in range(1, groups):
        coef_copy(step).start()
    coefs[grp] = packed_ref[...]

    if padded_len > krylov_len:
        for chunk in range(chunks):
            for which in range(2):
                fields[which, chunk, pl.ds(krylov_len, padded_len - krylov_len)] = jnp.zeros(
                    (padded_len - krylov_len, TILE, inner_dev), jnp.bfloat16
                )
    shape = spread.shape
    spread[...] = jnp.where(
        lax.shift_right_logical(grid_iota(shape, 1), 4) == grid_iota(shape, 0), 1.0, 0.0
    ).astype(jnp.bfloat16)

    for step in range(1, groups):
        coef_copy(step).wait()

    all_coefs = coefs[...].reshape(wanted, packed_width)
    shift_values = expand_rows(all_coefs[:, packed_width - 1 :], inner_dev)
    for part in range(cdiv(steps * TILE, LANES)):
        reps[part] = jnp.dot(
            all_coefs[:, part * LANES : (part + 1) * LANES].astype(jnp.bfloat16),
            spread[...],
            preferred_element_type=jnp.float32,
        )
    per_part = LANES // TILE
    same = (grid_iota((TILE, wide), 1) & (TILE - 1)) == grid_iota((TILE, wide), 0)
    for step in range(steps):
        at = (step % per_part) * wide
        values = reps[step // per_part, :, at : at + wide]
        values = jnp.where(same[None], values.reshape(wanted, 1, wide), 0.0)
        expanded[:, step * wide : (step + 1) * wide] = values.reshape(wanted * TILE, wide).astype(jnp.bfloat16)

    def data_copy(chunk, step):
        dest = lax.rem(grp + step, groups)
        return remote(
            coded.at[chunk, pl.ds(pl.multiple_of(dest * block, block), block)],
            coded_ref.at[grp, chunk],
            data_sems, (chunk, step), "grp", step,
        )

    def own_copy(chunk):
        return pltpu.make_async_copy(
            coded.at[chunk, pl.ds(pl.multiple_of(grp * block, block), block)],
            coded_ref.at[grp, chunk],
            own_sem.at[chunk],
        )

    def stat_copy(step):
        return remote(
            stat_send.at[lax.rem(grp + step, groups)], stat_recv.at[grp], stat_sems, (step,), "grp", step
        )

    def compute(chunk, stats):
        for copy in loads(chunk):
            copy.wait()
        both = jnp.concatenate(
            [fields[which, chunk].reshape(padded_len * TILE, inner_dev) for which in range(2)], axis=1
        )
        product = jnp.dot(expanded[...], both, preferred_element_type=jnp.float32)
        product = product.reshape(wanted, TILE, 2 * inner_dev)
        ritz = product[:, :, :inner_dev]
        resid = product[:, :, inner_dev:] - shift_values * ritz
        for kind, cols in enumerate((ritz, resid)):
            squares = jnp.sum(jnp.sum(cols * cols, axis=1), axis=1, keepdims=True)
            most = jnp.max(jnp.max(jnp.abs(cols), axis=1), axis=1, keepdims=True)
            most = jnp.maximum(most, LEAST)
            codes = jnp.exp(SLOPE * jnp.log(1.0 + jnp.abs(cols) * expand_rows(SPREAD / most, inner_dev)) - REACH)
            codes = jnp.where(cols < 0.0, -codes, codes)
            coded[chunk, :, kind * inner_dev : (kind + 1) * inner_dev] = codes.reshape(
                wanted * TILE, inner_dev
            ).astype(jnp.bfloat16)
            stats = jnp.where(lane_stats == 2 * chunk + kind, most, stats)
            stats = jnp.where(lane_stats == 2 * chunks + kind, stats + squares, stats)

        @pl.when(chunk == chunks - 1)
        def _():
            stat_send[...] = stats.reshape(groups, wanted_dev, LANES)
            for step in range(1, groups):
                stat_copy(step).start()

        for step in range(1, groups):
            data_copy(chunk, step).start()
        own_copy(chunk).start()
        return stats

    lax.fori_loop(0, chunks, compute, jnp.zeros((wanted, LANES), jnp.float32))

    for step in range(1, groups):
        stat_copy(step).wait()
    stat_recv[grp] = stat_send[grp]
    row_send[...] = jnp.sum(stat_recv[...], axis=0)

    def row_copy(step):
        return remote(row_send, row_recv.at[row], row_sems, (step,), "row", step)

    for step in range(1, rows):
        row_copy(step).start()
    stats_ref[...] = stat_recv[...]
    row_recv[row] = row_send[...]
    for step in range(1, rows):
        row_copy(step).wait()
    total_ref[...] = jnp.sum(row_recv[...], axis=0)

    def finish(chunk, carry):
        for step in range(1, groups):
            data_copy(chunk, step).wait()
        own_copy(chunk).wait()
        return carry

    lax.fori_loop(0, chunks, finish, 0)


def finish_kernel(rows_total, chunks, coded_ref, stats_ref, total_ref, ritz_ref, resid_ref, norm_ref):
    chunk = pl.program_id(0)
    groups, wanted_dev = stats_ref.shape[:2]
    inner_dev = coded_ref.shape[3] // 2
    lanes = grid_iota((wanted_dev, LANES), 1)

    def pick(tile, lane):
        return jnp.sum(jnp.where(lanes == lane, tile, 0.0), axis=1, keepdims=True)

    total = total_ref[...]
    ritz_squares = pick(total, 2 * chunks) + 1.0
    resid_squares = pick(total, 2 * chunks + 1)
    factor = jnp.sqrt(rows_total / ritz_squares)
    for source in range(groups):
        for kind, out_ref in enumerate((ritz_ref, resid_ref)):
            scale = pick(stats_ref[source], 2 * chunk + kind) * (factor * (1.0 / SPREAD))
            codes = coded_ref[source, 0, :, kind * inner_dev : (kind + 1) * inner_dev].astype(jnp.float32)
            size = jnp.exp((jnp.log(jnp.abs(codes)) + REACH) * (1.0 / SLOPE)) - 1.0
            size = jnp.where(codes < 0.0, -size, size)
            size = size.reshape(wanted_dev, TILE, inner_dev)
            out_ref[:, :, source * inner_dev : (source + 1) * inner_dev] = size * expand_rows(scale, inner_dev)
    norms = jnp.broadcast_to(jnp.sqrt(resid_squares / ritz_squares), (wanted_dev, LANES))
    diagonal = lanes == grid_iota((wanted_dev, LANES), 0)
    norm_ref[...] = jnp.sum(jnp.where(diagonal, norms, 0.0), axis=0, keepdims=True)


def body(groups, rows, krylov_basis, krylov_image, tridiag_vectors, ritz_values):
    krylov_len, outer_dev, inner_dev = krylov_basis.shape
    wanted_dev = tridiag_vectors.shape[1]
    wanted = groups * wanted_dev
    chunks = outer_dev // TILE
    block = wanted_dev * TILE
    padded_len = cdiv(krylov_len, TILE) * TILE
    packed_width = cdiv(padded_len + 1, LANES) * LANES
    rows_total = float(outer_dev * inner_dev * groups * rows)
    packed = jnp.concatenate(
        [
            tridiag_vectors.astype(jnp.float32).T,
            jnp.zeros((wanted_dev, packed_width - krylov_len - 1), jnp.float32),
            ritz_values.astype(jnp.float32)[:, None],
        ],
        axis=1,
    )
    f32, bf16 = jnp.float32, jnp.bfloat16
    dma = pltpu.SemaphoreType.DMA
    anywhere = pl.BlockSpec(memory_space=pl.ANY)
    vmem = pl.BlockSpec(memory_space=pltpu.VMEM)
    parts = cdiv(padded_len, LANES)
    coded, stats, total = pl.pallas_call(
        functools.partial(exchange_kernel, groups, rows, krylov_len),
        name="exchange",
        out_shape=(
            jax.ShapeDtypeStruct((groups, chunks, block, 2 * inner_dev), bf16),
            jax.ShapeDtypeStruct((groups, wanted_dev, LANES), f32),
            jax.ShapeDtypeStruct((wanted_dev, LANES), f32),
        ),
        in_specs=[vmem, anywhere, anywhere],
        out_specs=(anywhere, vmem, vmem),
        scratch_shapes=[
            pltpu.VMEM((groups, wanted_dev, packed_width), f32),
            pltpu.VMEM((2, chunks, padded_len, TILE, inner_dev), bf16),
            pltpu.VMEM((LANES, LANES * TILE), bf16),
            pltpu.VMEM((parts, wanted, LANES * TILE), f32),
            pltpu.VMEM((wanted * TILE, padded_len * TILE), bf16),
            pltpu.VMEM((chunks, wanted * TILE, 2 * inner_dev), bf16),
            pltpu.VMEM((groups, wanted_dev, LANES), f32),
            pltpu.VMEM((groups, wanted_dev, LANES), f32),
            pltpu.VMEM((wanted_dev, LANES), f32),
            pltpu.VMEM((rows, wanted_dev, LANES), f32),
            dma((2, chunks)),
            dma((2, groups)),
            dma((2, chunks, groups)),
            dma((chunks,)),
            dma((2, groups)),
            dma((2, rows)),
        ],
        compiler_params=pltpu.CompilerParams(
            collective_id=0, has_side_effects=True, vmem_limit_bytes=48 * 1024 * 1024
        ),
    )(packed, krylov_basis, krylov_image)
    ritz_vectors, ritz_residuals, norms = pl.pallas_call(
        functools.partial(finish_kernel, rows_total, chunks),
        name="finish",
        grid=(chunks,),
        out_shape=(
            jax.ShapeDtypeStruct((wanted_dev, outer_dev, groups * inner_dev), f32),
            jax.ShapeDtypeStruct((wanted_dev, outer_dev, groups * inner_dev), f32),
            jax.ShapeDtypeStruct((1, LANES), f32),
        ),
        in_specs=[
            pl.BlockSpec((groups, 1, block, 2 * inner_dev), lambda c: (0, c, 0, 0)),
            pl.BlockSpec((groups, wanted_dev, LANES), lambda c: (0, 0, 0)),
            pl.BlockSpec((wanted_dev, LANES), lambda c: (0, 0)),
        ],
        out_specs=(
            pl.BlockSpec((wanted_dev, TILE, groups * inner_dev), lambda c: (0, c, 0)),
            pl.BlockSpec((wanted_dev, TILE, groups * inner_dev), lambda c: (0, c, 0)),
            pl.BlockSpec((1, LANES), lambda c: (0, 0)),
        ),
    )(coded, stats, total)
    return ritz_vectors, ritz_residuals, norms[0, :wanted_dev]


def solution(mesh):
    placed = (P(None, "row", "grp"), P(None, "row", "grp"), P(None, "grp"), P("grp"))
    return jax.shard_map(
        functools.partial(body, mesh.shape["grp"], mesh.shape["row"]),
        mesh=mesh,
        in_specs=placed,
        out_specs=(P("grp", "row", None), P("grp", "row", None), P("grp")),
        check_vma=False,
    )
```

```python
import functools
import math

import jax
import jax.numpy as jnp
from jax import lax
from jax.experimental import pallas as pl
from jax.experimental.pallas import tpu as pltpu
from jax.sharding import PartitionSpec as P

MESH = pl.DeviceIdType.MESH
MIB = 1 << 20
TILE = 16
LANES = 128
SPREAD = 256.0
REACH = 86.0
SLOPE = 2.0 * REACH / math.log(1.0 + SPREAD)
LEAST = 1e-35


def cdiv(a, b):
    return (a + b - 1) // b


def grid_iota(shape, dim):
    return lax.broadcasted_iota(jnp.int32, shape, dim)


def expand_rows(cols, width):
    return jnp.broadcast_to(cols, (cols.shape[0], width)).reshape(cols.shape[0], 1, width)


def exchange_kernel(
    groups, rows, krylov_len,
    tridiag_ref, values_ref, basis_ref, image_ref,
    coded_ref, stats_ref, total_ref,
    packed_ref, coefs, fields, spread, reps, expanded, coded, stat_send, stat_recv, row_send, row_recv,
    load_sem, coef_sems, data_sems, own_sem, stat_sems, row_sems,
):
    wanted_dev, packed_width = packed_ref.shape
    wanted = groups * wanted_dev
    chunks = fields.shape[1]
    inner_dev = basis_ref.shape[2]
    padded_len = fields.shape[2]
    steps = padded_len // TILE
    wide = TILE * TILE
    block = wanted_dev * TILE
    grp = lax.axis_index("grp")
    row = lax.axis_index("row")
    lane_stats = grid_iota((wanted, LANES), 1)

    def loads(chunk):
        span = pl.ds(pl.multiple_of(chunk * TILE, TILE), TILE)
        return [
            pltpu.make_async_copy(
                ref.at[:, span, :], fields.at[which, chunk, pl.ds(0, krylov_len)], load_sem.at[which, chunk]
            )
            for which, ref in enumerate((basis_ref, image_ref))
        ]

    for chunk in range(chunks):
        for copy in loads(chunk):
            copy.start()

    near = grid_iota((wanted_dev, wanted_dev), 0) == grid_iota((wanted_dev, wanted_dev), 1)
    own_values = jnp.broadcast_to(values_ref[...].astype(jnp.float32), (wanted_dev, wanted_dev))
    own_values = jnp.sum(jnp.where(near, own_values, 0.0), axis=1, keepdims=True)
    packed_ref[...] = jnp.broadcast_to(own_values, (wanted_dev, packed_width))
    packed_ref[:, :krylov_len] = tridiag_ref[...].astype(jnp.float32)

    barrier = pltpu.get_barrier_semaphore()
    for step in range(1, groups):
        pl.semaphore_signal(barrier, inc=1, device_id={"grp": lax.rem(grp + step, groups)}, device_id_type=MESH)
    for step in range(1, rows):
        pl.semaphore_signal(barrier, inc=1, device_id={"row": lax.rem(row + step, rows)}, device_id_type=MESH)
    pl.semaphore_wait(barrier, groups + rows - 2)

    def remote(src, dst, sems, index, axis, step):
        me, size = (grp, groups) if axis == "grp" else (row, rows)
        return pltpu.make_async_remote_copy(
            src_ref=src,
            dst_ref=dst,
            send_sem=sems.at[(0,) + index],
            recv_sem=sems.at[(1,) + index],
            device_id={axis: lax.rem(me + step, size)},
            device_id_type=MESH,
        )

    def coef_copy(step):
        return remote(packed_ref, coefs.at[grp], coef_sems, (step,), "grp", step)

    for step in range(1, groups):
        coef_copy(step).start()
    coefs[grp] = packed_ref[...]

    if padded_len > krylov_len:
        for chunk in range(chunks):
            for which in range(2):
                fields[which, chunk, pl.ds(krylov_len, padded_len - krylov_len)] = jnp.zeros(
                    (padded_len - krylov_len, TILE, inner_dev), jnp.bfloat16
                )
    shape = spread.shape
    spread[...] = jnp.where(
        lax.shift_right_logical(grid_iota(shape, 1), 4) == grid_iota(shape, 0), 1.0, 0.0
    ).astype(jnp.bfloat16)

    for step in range(1, groups):
        coef_copy(step).wait()

    all_coefs = coefs[...].reshape(wanted, packed_width)
    shift_values = expand_rows(all_coefs[:, packed_width - 1 :], inner_dev)
    for part in range(cdiv(steps * TILE, LANES)):
        reps[part] = jnp.dot(
            all_coefs[:, part * LANES : (part + 1) * LANES].astype(jnp.bfloat16),
            spread[...],
            preferred_element_type=jnp.float32,
        )
    per_part = LANES // TILE
    same = (grid_iota((TILE, wide), 1) & (TILE - 1)) == grid_iota((TILE, wide), 0)
    for step in range(steps):
        at = (step % per_part) * wide
        values = reps[step // per_part, :, at : at + wide]
        values = jnp.where(same[None], values.reshape(wanted, 1, wide), 0.0)
        expanded[:, step * wide : (step + 1) * wide] = values.reshape(wanted * TILE, wide).astype(jnp.bfloat16)

    def data_copy(chunk, step):
        dest = lax.rem(grp + step, groups)
        return remote(
            coded.at[chunk, pl.ds(pl.multiple_of(dest * block, block), block)],
            coded_ref.at[grp, chunk],
            data_sems, (chunk, step), "grp", step,
        )

    def own_copy(chunk):
        return pltpu.make_async_copy(
            coded.at[chunk, pl.ds(pl.multiple_of(grp * block, block), block)],
            coded_ref.at[grp, chunk],
            own_sem.at[chunk],
        )

    def stat_copy(step):
        return remote(
            stat_send.at[lax.rem(grp + step, groups)], stat_recv.at[grp], stat_sems, (step,), "grp", step
        )

    def compute(chunk, stats):
        for copy in loads(chunk):
            copy.wait()
        both = jnp.concatenate(
            [fields[which, chunk].reshape(padded_len * TILE, inner_dev) for which in range(2)], axis=1
        )
        product = jnp.dot(expanded[...], both, preferred_element_type=jnp.float32)
        product = product.reshape(wanted, TILE, 2 * inner_dev)
        ritz = product[:, :, :inner_dev]
        resid = product[:, :, inner_dev:] - shift_values * ritz
        for kind, cols in enumerate((ritz, resid)):
            squares = jnp.sum(jnp.sum(cols * cols, axis=1), axis=1, keepdims=True)
            most = jnp.max(jnp.max(jnp.abs(cols), axis=1), axis=1, keepdims=True)
            most = jnp.maximum(most, LEAST)
            codes = jnp.exp(SLOPE * jnp.log(1.0 + jnp.abs(cols) * expand_rows(SPREAD / most, inner_dev)) - REACH)
            codes = jnp.where(cols < 0.0, -codes, codes)
            coded[chunk, :, kind * inner_dev : (kind + 1) * inner_dev] = codes.reshape(
                wanted * TILE, inner_dev
            ).astype(jnp.bfloat16)
            stats = jnp.where(lane_stats == 2 * chunk + kind, most, stats)
            stats = jnp.where(lane_stats == 2 * chunks + kind, stats + squares, stats)

        @pl.when(chunk == chunks - 1)
        def _():
            stat_send[...] = stats.reshape(groups, wanted_dev, LANES)
            for step in range(1, groups):
                stat_copy(step).start()

        for step in range(1, groups):
            data_copy(chunk, step).start()
        own_copy(chunk).start()
        return stats

    lax.fori_loop(0, chunks, compute, jnp.zeros((wanted, LANES), jnp.float32))

    for step in range(1, groups):
        stat_copy(step).wait()
    stat_recv[grp] = stat_send[grp]
    row_send[...] = jnp.sum(stat_recv[...], axis=0)

    def row_copy(step):
        return remote(row_send, row_recv.at[row], row_sems, (step,), "row", step)

    for step in range(1, rows):
        row_copy(step).start()
    stats_ref[...] = stat_recv[...]
    row_recv[row] = row_send[...]
    for step in range(1, rows):
        row_copy(step).wait()
    total_ref[...] = jnp.sum(row_recv[...], axis=0)

    def finish(chunk, carry):
        for step in range(1, groups):
            data_copy(chunk, step).wait()
        own_copy(chunk).wait()
        return carry

    lax.fori_loop(0, chunks, finish, 0)


def finish_kernel(rows_total, chunks, coded_ref, stats_ref, total_ref, ritz_ref, resid_ref, norm_ref):
    chunk = pl.program_id(0)
    groups, wanted_dev = stats_ref.shape[:2]
    inner_dev = coded_ref.shape[3] // 2
    lanes = grid_iota((wanted_dev, LANES), 1)

    def pick(tile, lane):
        return jnp.sum(jnp.where(lanes == lane, tile, 0.0), axis=1, keepdims=True)

    total = total_ref[...]
    ritz_squares = pick(total, 2 * chunks) + 1.0
    resid_squares = pick(total, 2 * chunks + 1)
    factor = jnp.sqrt(rows_total / ritz_squares)
    for source in range(groups):
        for kind, out_ref in enumerate((ritz_ref, resid_ref)):
            scale = pick(stats_ref[source], 2 * chunk + kind) * (factor * (1.0 / SPREAD))
            codes = coded_ref[source, 0, :, kind * inner_dev : (kind + 1) * inner_dev].astype(jnp.float32)
            size = jnp.exp((jnp.log(jnp.abs(codes)) + REACH) * (1.0 / SLOPE)) - 1.0
            size = jnp.where(codes < 0.0, -size, size)
            size = size.reshape(wanted_dev, TILE, inner_dev)
            out_ref[:, :, source * inner_dev : (source + 1) * inner_dev] = size * expand_rows(scale, inner_dev)
    norms = jnp.broadcast_to(jnp.sqrt(resid_squares / ritz_squares), (wanted_dev, LANES))
    diagonal = lanes == grid_iota((wanted_dev, LANES), 0)
    norm_ref[...] = jnp.sum(jnp.where(diagonal, norms, 0.0), axis=0)[:wanted_dev]


def body(groups, rows, krylov_basis, krylov_image, tridiag_vectors, ritz_values):
    krylov_len, outer_dev, inner_dev = krylov_basis.shape
    wanted_dev = tridiag_vectors.shape[1]
    wanted = groups * wanted_dev
    chunks = outer_dev // TILE
    block = wanted_dev * TILE
    padded_len = cdiv(krylov_len, TILE) * TILE
    packed_width = cdiv(padded_len + 1, LANES) * LANES
    rows_total = float(outer_dev * inner_dev * groups * rows)
    f32, bf16 = jnp.float32, jnp.bfloat16
    dma = pltpu.SemaphoreType.DMA
    anywhere = pl.BlockSpec(memory_space=pl.ANY)
    vmem = pl.BlockSpec(memory_space=pltpu.VMEM)
    hbm = pl.BlockSpec(memory_space=pltpu.HBM)
    parts = cdiv(padded_len, LANES)
    coded, stats, total = pl.pallas_call(
        functools.partial(exchange_kernel, groups, rows, krylov_len),
        name="exchange",
        out_shape=(
            jax.ShapeDtypeStruct((groups, chunks, block, 2 * inner_dev), bf16),
            jax.ShapeDtypeStruct((groups, wanted_dev, LANES), f32),
            jax.ShapeDtypeStruct((wanted_dev, LANES), f32),
        ),
        in_specs=[vmem, vmem, hbm, hbm],
        out_specs=(anywhere, vmem, vmem),
        scratch_shapes=[
            pltpu.VMEM((wanted_dev, packed_width), f32),
            pltpu.VMEM((groups, wanted_dev, packed_width), f32),
            pltpu.VMEM((2, chunks, padded_len, TILE, inner_dev), bf16),
            pltpu.VMEM((LANES, LANES * TILE), bf16),
            pltpu.VMEM((parts, wanted, LANES * TILE), f32),
            pltpu.VMEM((wanted * TILE, padded_len * TILE), bf16),
            pltpu.VMEM((chunks, wanted * TILE, 2 * inner_dev), bf16),
            pltpu.VMEM((groups, wanted_dev, LANES), f32),
            pltpu.VMEM((groups, wanted_dev, LANES), f32),
            pltpu.VMEM((wanted_dev, LANES), f32),
            pltpu.VMEM((rows, wanted_dev, LANES), f32),
            dma((2, chunks)),
            dma((2, groups)),
            dma((2, chunks, groups)),
            dma((chunks,)),
            dma((2, groups)),
            dma((2, rows)),
        ],
        compiler_params=pltpu.CompilerParams(
            collective_id=0, has_side_effects=True, vmem_limit_bytes=61 * MIB
        ),
    )(tridiag_vectors.T, ritz_values[None], krylov_basis, krylov_image)
    ritz_vectors, ritz_residuals, norms = pl.pallas_call(
        functools.partial(finish_kernel, rows_total, chunks),
        name="finish",
        grid=(chunks,),
        out_shape=(
            jax.ShapeDtypeStruct((wanted_dev, outer_dev, groups * inner_dev), f32),
            jax.ShapeDtypeStruct((wanted_dev, outer_dev, groups * inner_dev), f32),
            jax.ShapeDtypeStruct((wanted_dev,), f32),
        ),
        in_specs=[
            pl.BlockSpec((groups, 1, block, 2 * inner_dev), lambda c: (0, c, 0, 0)),
            pl.BlockSpec((groups, wanted_dev, LANES), lambda c: (0, 0, 0)),
            pl.BlockSpec((wanted_dev, LANES), lambda c: (0, 0)),
        ],
        out_specs=(
            pl.BlockSpec((wanted_dev, TILE, groups * inner_dev), lambda c: (0, c, 0)),
            pl.BlockSpec((wanted_dev, TILE, groups * inner_dev), lambda c: (0, c, 0)),
            pl.BlockSpec((wanted_dev,), lambda c: (0,)),
        ),
        compiler_params=pltpu.CompilerParams(vmem_limit_bytes=16 * MIB),
    )(coded, stats, total)
    return ritz_vectors, ritz_residuals, norms


def solution(mesh):
    placed = (P(None, "row", "grp"), P(None, "row", "grp"), P(None, "grp"), P("grp"))
    return jax.shard_map(
        functools.partial(body, mesh.shape["grp"], mesh.shape["row"]),
        mesh=mesh,
        in_specs=placed,
        out_specs=(P("grp", "row", None), P("grp", "row", None), P("grp")),
        check_vma=False,
    )
```

```python
import functools
import math

import jax
import jax.numpy as jnp
from jax import lax
from jax.experimental import pallas as pl
from jax.experimental.pallas import tpu as pltpu
from jax.sharding import PartitionSpec as P

MESH = pl.DeviceIdType.MESH
MIB = 1 << 20
TILE = 8
STEP = 16
LANES = 128
SPREAD = 256.0
REACH = 86.0
SLOPE = 2.0 * REACH / math.log(1.0 + SPREAD)
LEAST = 1e-35


def cdiv(a, b):
    return (a + b - 1) // b


def grid_iota(shape, dim):
    return lax.broadcasted_iota(jnp.int32, shape, dim)


def expand_rows(cols, width):
    return jnp.broadcast_to(cols, (cols.shape[0], width)).reshape(cols.shape[0], 1, width)


def exchange_kernel(
    groups, rows, krylov_len,
    tridiag_ref, values_ref, basis_ref, image_ref,
    coded_ref, stats_ref, total_ref,
    packed_ref, coefs, fields, spread, reps, expanded, coded, stat_send, stat_recv, square_send, square_recv,
    load_sem, coef_sems, data_sems, own_sem, stat_sems, square_sems,
):
    wanted_dev, packed_width = packed_ref.shape
    wanted = groups * wanted_dev
    chunks = fields.shape[1]
    inner_dev = basis_ref.shape[2]
    padded_len = fields.shape[2]
    steps = padded_len // STEP
    wide = STEP * TILE
    block = wanted_dev * TILE
    grp = lax.axis_index("grp")
    row = lax.axis_index("row")
    lane_stats = grid_iota((wanted, LANES), 1)

    def loads(chunk):
        span = pl.ds(pl.multiple_of(chunk * TILE, TILE), TILE)
        return [
            pltpu.make_async_copy(
                ref.at[:, span, :], fields.at[which, chunk, pl.ds(0, krylov_len)], load_sem.at[which, chunk]
            )
            for which, ref in enumerate((basis_ref, image_ref))
        ]

    for chunk in range(chunks):
        for copy in loads(chunk):
            copy.start()

    near = grid_iota((wanted_dev, wanted_dev), 0) == grid_iota((wanted_dev, wanted_dev), 1)
    own_values = jnp.broadcast_to(values_ref[...].astype(jnp.float32), (wanted_dev, wanted_dev))
    own_values = jnp.sum(jnp.where(near, own_values, 0.0), axis=1, keepdims=True)
    packed_ref[...] = jnp.broadcast_to(own_values, (wanted_dev, packed_width))
    packed_ref[:, :krylov_len] = tridiag_ref[...].astype(jnp.float32)

    barrier = pltpu.get_barrier_semaphore()
    def others(action):
        for across in range(groups):
            lax.fori_loop(1 if across == 0 else 0, rows, functools.partial(action, across), 0)

    def device(across, along):
        return {"grp": lax.rem(grp + across, groups), "row": lax.rem(row + along, rows)}

    def greet(across, along, carry):
        pl.semaphore_signal(barrier, inc=1, device_id=device(across, along), device_id_type=MESH)
        return carry

    others(greet)
    pl.semaphore_wait(barrier, groups * rows - 1)

    def remote(src, dst, sems, index, across, along=0):
        return pltpu.make_async_remote_copy(
            src_ref=src,
            dst_ref=dst,
            send_sem=sems.at[(0,) + index],
            recv_sem=sems.at[(1,) + index],
            device_id=device(across, along),
            device_id_type=MESH,
        )

    def coef_copy(step):
        return remote(packed_ref, coefs.at[grp], coef_sems, (step,), step)

    for step in range(1, groups):
        coef_copy(step).start()
    coefs[grp] = packed_ref[...]

    if padded_len > krylov_len:
        for chunk in range(chunks):
            for which in range(2):
                fields[which, chunk, pl.ds(krylov_len, padded_len - krylov_len)] = jnp.zeros(
                    (padded_len - krylov_len, TILE, inner_dev), jnp.bfloat16
                )
    shape = spread.shape
    spread[...] = jnp.where(
        lax.shift_right_logical(grid_iota(shape, 1), 3) == grid_iota(shape, 0), 1.0, 0.0
    ).astype(jnp.bfloat16)

    for step in range(1, groups):
        coef_copy(step).wait()

    all_coefs = coefs[...].reshape(wanted, packed_width)
    shift_values = expand_rows(all_coefs[:, packed_width - 1 :], inner_dev)
    for part in range(cdiv(padded_len, LANES)):
        reps[part] = jnp.dot(
            all_coefs[:, part * LANES : (part + 1) * LANES].astype(jnp.bfloat16),
            spread[...],
            preferred_element_type=jnp.float32,
        )
    per_part = LANES // STEP
    same = (grid_iota((TILE, wide), 1) & (TILE - 1)) == grid_iota((TILE, wide), 0)
    for step in range(steps):
        at = (step % per_part) * wide
        values = reps[step // per_part, :, at : at + wide]
        values = jnp.where(same[None], values.reshape(wanted, 1, wide), 0.0)
        expanded[:, step * wide : (step + 1) * wide] = values.reshape(wanted * TILE, wide).astype(jnp.bfloat16)

    def data_copy(chunk, step):
        dest = lax.rem(grp + step, groups)
        return remote(
            coded.at[chunk, pl.ds(pl.multiple_of(dest * block, block), block)],
            coded_ref.at[grp, chunk],
            data_sems, (chunk, step), step,
        )

    def own_copy(chunk):
        return pltpu.make_async_copy(
            coded.at[chunk, pl.ds(pl.multiple_of(grp * block, block), block)],
            coded_ref.at[grp, chunk],
            own_sem.at[chunk],
        )

    def stat_copy(step):
        return remote(
            stat_send.at[lax.rem(grp + step, groups)], stat_recv.at[grp], stat_sems, (step,), step
        )

    def square_copy(across, along):
        return remote(
            square_send.at[lax.rem(grp + across, groups)], square_recv.at[grp * rows + row],
            square_sems, (across, along), across, along,
        )

    def square_start(across, along, carry):
        square_copy(across, along).start()
        return carry

    def square_wait(across, along, carry):
        square_copy(across, along).wait()
        return carry

    column = grid_iota((wanted, LANES), 0) % wanted_dev

    def compute(chunk, carry):
        stats, sums = carry
        for copy in loads(chunk):
            copy.wait()
        both = jnp.concatenate(
            [fields[which, chunk].reshape(padded_len * TILE, inner_dev) for which in range(2)], axis=1
        )
        product = jnp.dot(expanded[...], both, preferred_element_type=jnp.float32)
        product = product.reshape(wanted, TILE, 2 * inner_dev)
        ritz = product[:, :, :inner_dev]
        resid = product[:, :, inner_dev:] - shift_values * ritz
        for kind, cols in enumerate((ritz, resid)):
            squares = jnp.sum(jnp.sum(cols * cols, axis=1), axis=1, keepdims=True)
            most = jnp.max(jnp.max(jnp.abs(cols), axis=1), axis=1, keepdims=True)
            most = jnp.maximum(most, LEAST)
            codes = jnp.exp(SLOPE * jnp.log(1.0 + jnp.abs(cols) * expand_rows(SPREAD / most, inner_dev)) - REACH)
            codes = jnp.where(cols < 0.0, -codes, codes)
            coded[chunk, :, kind * inner_dev : (kind + 1) * inner_dev] = codes.reshape(
                wanted * TILE, inner_dev
            ).astype(jnp.bfloat16)
            stats = jnp.where(lane_stats == 2 * chunk + kind, most, stats)
            sums = jnp.where(lane_stats == column + kind * wanted_dev, sums + squares, sums)

        @pl.when(chunk == chunks - 1)
        def _():
            square_send[...] = jnp.sum(sums.reshape(groups, wanted_dev, LANES), axis=1, keepdims=True)
            others(square_start)
            stat_send[...] = stats.reshape(groups, wanted_dev, LANES)
            for step in range(1, groups):
                stat_copy(step).start()

        for step in range(1, groups):
            data_copy(chunk, step).start()
        own_copy(chunk).start()
        return stats, sums

    nothing = jnp.zeros((wanted, LANES), jnp.float32)
    lax.fori_loop(0, chunks, compute, (nothing, nothing))

    for step in range(1, groups):
        stat_copy(step).wait()
    stat_recv[grp] = stat_send[grp]
    stats_ref[...] = stat_recv[...]
    others(square_wait)
    square_recv[grp * rows + row] = square_send[grp]
    total_ref[...] = jnp.sum(square_recv[...], axis=0)

    def finish(chunk, carry):
        for step in range(1, groups):
            data_copy(chunk, step).wait()
        own_copy(chunk).wait()
        return carry

    lax.fori_loop(0, chunks, finish, 0)


def finish_kernel(rows_total, coded_ref, stats_ref, total_ref, ritz_ref, resid_ref, norm_ref):
    groups, wanted_dev = stats_ref.shape[:2]
    several = coded_ref.shape[1]
    first = pl.program_id(0) * several
    inner_dev = coded_ref.shape[3] // 2
    lanes = grid_iota((wanted_dev, LANES), 1)
    columns = grid_iota((wanted_dev, LANES), 0)

    def pick(tile, lane):
        return jnp.sum(jnp.where(lanes == lane, tile, 0.0), axis=1, keepdims=True)

    total = jnp.broadcast_to(total_ref[...], (wanted_dev, LANES))
    ritz_squares = pick(total, columns) + 1.0
    resid_squares = pick(total, columns + wanted_dev)
    factor = jnp.sqrt(rows_total / ritz_squares)
    for source in range(groups):
        for part in range(several):
            for kind, out_ref in enumerate((ritz_ref, resid_ref)):
                scale = pick(stats_ref[source], 2 * (first + part) + kind) * (factor * (1.0 / SPREAD))
                codes = coded_ref[source, part, :, kind * inner_dev : (kind + 1) * inner_dev].astype(jnp.float32)
                size = jnp.exp((jnp.log(jnp.abs(codes)) + REACH) * (1.0 / SLOPE)) - 1.0
                size = jnp.where(codes < 0.0, -size, size)
                size = size.reshape(wanted_dev, TILE, inner_dev) * expand_rows(scale, inner_dev)
                out_ref[:, part * TILE : (part + 1) * TILE, source * inner_dev : (source + 1) * inner_dev] = size
    norms = jnp.broadcast_to(jnp.sqrt(resid_squares / ritz_squares), (wanted_dev, LANES))
    norm_ref[...] = jnp.sum(jnp.where(lanes == columns, norms, 0.0), axis=0)[:wanted_dev]


def body(groups, rows, krylov_basis, krylov_image, tridiag_vectors, ritz_values):
    krylov_len, outer_dev, inner_dev = krylov_basis.shape
    wanted_dev = tridiag_vectors.shape[1]
    wanted = groups * wanted_dev
    chunks = outer_dev // TILE
    block = wanted_dev * TILE
    padded_len = cdiv(krylov_len, STEP) * STEP
    packed_width = cdiv(padded_len + 1, LANES) * LANES
    rows_total = float(outer_dev * inner_dev * groups * rows)
    f32, bf16 = jnp.float32, jnp.bfloat16
    dma = pltpu.SemaphoreType.DMA
    anywhere = pl.BlockSpec(memory_space=pl.ANY)
    vmem = pl.BlockSpec(memory_space=pltpu.VMEM)
    hbm = pl.BlockSpec(memory_space=pltpu.HBM)
    parts = cdiv(padded_len, LANES)
    several = 2 if chunks % 2 == 0 else 1
    coded, stats, total = pl.pallas_call(
        functools.partial(exchange_kernel, groups, rows, krylov_len),
        name="exchange",
        out_shape=(
            jax.ShapeDtypeStruct((groups, chunks, block, 2 * inner_dev), bf16),
            jax.ShapeDtypeStruct((groups, wanted_dev, LANES), f32),
            jax.ShapeDtypeStruct((1, LANES), f32),
        ),
        in_specs=[vmem, vmem, hbm, hbm],
        out_specs=(anywhere, vmem, vmem),
        scratch_shapes=[
            pltpu.VMEM((wanted_dev, packed_width), f32),
            pltpu.VMEM((groups, wanted_dev, packed_width), f32),
            pltpu.VMEM((2, chunks, padded_len, TILE, inner_dev), bf16),
            pltpu.VMEM((LANES, LANES * TILE), bf16),
            pltpu.VMEM((parts, wanted, LANES * TILE), f32),
            pltpu.VMEM((wanted * TILE, padded_len * TILE), bf16),
            pltpu.VMEM((chunks, wanted * TILE, 2 * inner_dev), bf16),
            pltpu.VMEM((groups, wanted_dev, LANES), f32),
            pltpu.VMEM((groups, wanted_dev, LANES), f32),
            pltpu.VMEM((groups, 1, LANES), f32),
            pltpu.VMEM((groups * rows, 1, LANES), f32),
            dma((2, chunks)),
            dma((2, groups)),
            dma((2, chunks, groups)),
            dma((chunks,)),
            dma((2, groups)),
            dma((2, groups, rows)),
        ],
        compiler_params=pltpu.CompilerParams(
            collective_id=0, has_side_effects=True, vmem_limit_bytes=60 * MIB
        ),
    )(tridiag_vectors.T, ritz_values[None], krylov_basis, krylov_image)
    ritz_vectors, ritz_residuals, norms = pl.pallas_call(
        functools.partial(finish_kernel, rows_total),
        name="finish",
        grid=(chunks // several,),
        out_shape=(
            jax.ShapeDtypeStruct((wanted_dev, outer_dev, groups * inner_dev), f32),
            jax.ShapeDtypeStruct((wanted_dev, outer_dev, groups * inner_dev), f32),
            jax.ShapeDtypeStruct((wanted_dev,), f32),
        ),
        in_specs=[
            pl.BlockSpec((groups, several, block, 2 * inner_dev), lambda c: (0, c, 0, 0)),
            pl.BlockSpec((groups, wanted_dev, LANES), lambda c: (0, 0, 0)),
            pl.BlockSpec((1, LANES), lambda c: (0, 0)),
        ],
        out_specs=(
            pl.BlockSpec((wanted_dev, several * TILE, groups * inner_dev), lambda c: (0, c, 0)),
            pl.BlockSpec((wanted_dev, several * TILE, groups * inner_dev), lambda c: (0, c, 0)),
            pl.BlockSpec((wanted_dev,), lambda c: (0,)),
        ),
        compiler_params=pltpu.CompilerParams(vmem_limit_bytes=16 * MIB),
    )(coded, stats, total)
    return ritz_vectors, ritz_residuals, norms


def solution(mesh):
    placed = (P(None, "row", "grp"), P(None, "row", "grp"), P(None, "grp"), P("grp"))
    return jax.shard_map(
        functools.partial(body, mesh.shape["grp"], mesh.shape["row"]),
        mesh=mesh,
        in_specs=placed,
        out_specs=(P("grp", "row", None), P("grp", "row", None), P("grp")),
        check_vma=False,
    )
```

```python
import functools
import math

import jax
import jax.numpy as jnp
from jax import lax
from jax.experimental import pallas as pl
from jax.experimental.pallas import tpu as pltpu
from jax.sharding import PartitionSpec as P

MESH = pl.DeviceIdType.MESH
MIB = 1 << 20
TILE = 8
STEP = 16
LANES = 128
SPREAD = 256.0
REACH = 86.0
SLOPE = 2.0 * REACH / math.log(1.0 + SPREAD)
LEAST = 1e-35


def cdiv(a, b):
    return (a + b - 1) // b


def grid_iota(shape, dim):
    return lax.broadcasted_iota(jnp.int32, shape, dim)


def expand_rows(cols, width):
    return jnp.broadcast_to(cols, (cols.shape[0], width)).reshape(cols.shape[0], 1, width)


def exchange_kernel(
    groups, rows, krylov_len,
    tridiag_ref, values_ref, basis_ref, image_ref,
    coded_ref, stats_ref, total_ref,
    packed_ref, coefs, fields, spread, reps, expanded, coded, stat_send, stat_recv, square_send, square_recv,
    load_sem, coef_sems, data_sems, own_sem, stat_sems, square_sems,
):
    wanted_dev, packed_width = packed_ref.shape
    wanted = groups * wanted_dev
    chunks = fields.shape[1]
    inner_dev = basis_ref.shape[2]
    padded_len = fields.shape[2]
    steps = padded_len // STEP
    wide = STEP * TILE
    block = wanted_dev * TILE
    grp = lax.axis_index("grp")
    row = lax.axis_index("row")
    lane_stats = grid_iota((wanted, LANES), 1)

    def loads(chunk):
        span = pl.ds(pl.multiple_of(chunk * TILE, TILE), TILE)
        return [
            pltpu.make_async_copy(
                ref.at[:, span, :], fields.at[which, chunk, pl.ds(0, krylov_len)], load_sem.at[which, chunk]
            )
            for which, ref in enumerate((basis_ref, image_ref))
        ]

    for chunk in range(chunks):
        for copy in loads(chunk):
            copy.start()

    near = grid_iota((wanted_dev, wanted_dev), 0) == grid_iota((wanted_dev, wanted_dev), 1)
    own_values = jnp.broadcast_to(values_ref[...].astype(jnp.float32), (wanted_dev, wanted_dev))
    own_values = jnp.sum(jnp.where(near, own_values, 0.0), axis=1, keepdims=True)
    packed_ref[...] = jnp.broadcast_to(own_values, (wanted_dev, packed_width))
    packed_ref[:, :krylov_len] = tridiag_ref[...].astype(jnp.float32)

    barrier = pltpu.get_barrier_semaphore()
    def others(action):
        for across in range(groups):
            lax.fori_loop(1 if across == 0 else 0, rows, functools.partial(action, across), 0)

    def device(across, along):
        return {"grp": lax.rem(grp + across, groups), "row": lax.rem(row + along, rows)}

    def greet(across, along, carry):
        pl.semaphore_signal(barrier, inc=1, device_id=device(across, along), device_id_type=MESH)
        return carry

    others(greet)
    pl.semaphore_wait(barrier, groups * rows - 1)

    def remote(src, dst, sems, index, across, along=0):
        return pltpu.make_async_remote_copy(
            src_ref=src,
            dst_ref=dst,
            send_sem=sems.at[(0,) + index],
            recv_sem=sems.at[(1,) + index],
            device_id=device(across, along),
            device_id_type=MESH,
        )

    def coef_copy(step):
        return remote(packed_ref, coefs.at[grp], coef_sems, (step,), step)

    for step in range(1, groups):
        coef_copy(step).start()
    coefs[grp] = packed_ref[...]

    if padded_len > krylov_len:
        for chunk in range(chunks):
            for which in range(2):
                fields[which, chunk, pl.ds(krylov_len, padded_len - krylov_len)] = jnp.zeros(
                    (padded_len - krylov_len, TILE, inner_dev), jnp.bfloat16
                )
    shape = spread.shape
    spread[...] = jnp.where(
        lax.shift_right_logical(grid_iota(shape, 1), 3) == grid_iota(shape, 0), 1.0, 0.0
    ).astype(jnp.bfloat16)

    for step in range(1, groups):
        coef_copy(step).wait()

    all_coefs = coefs[...].reshape(wanted, packed_width)
    shift_values = expand_rows(all_coefs[:, packed_width - 1 :], inner_dev)
    for part in range(cdiv(padded_len, LANES)):
        reps[part] = jnp.dot(
            all_coefs[:, part * LANES : (part + 1) * LANES].astype(jnp.bfloat16),
            spread[...],
            preferred_element_type=jnp.float32,
        )
    per_part = LANES // STEP
    same = (grid_iota((TILE, wide), 1) & (TILE - 1)) == grid_iota((TILE, wide), 0)
    for step in range(steps):
        at = (step % per_part) * wide
        values = reps[step // per_part, :, at : at + wide]
        values = jnp.where(same[None], values.reshape(wanted, 1, wide), 0.0)
        expanded[:, step * wide : (step + 1) * wide] = values.reshape(wanted * TILE, wide).astype(jnp.bfloat16)

    def data_copy(chunk, step):
        dest = lax.rem(grp + step, groups)
        return remote(
            coded.at[chunk, pl.ds(pl.multiple_of(dest * block, block), block)],
            coded_ref.at[grp, chunk],
            data_sems, (chunk, step), step,
        )

    def own_copy(chunk):
        return pltpu.make_async_copy(
            coded.at[chunk, pl.ds(pl.multiple_of(grp * block, block), block)],
            coded_ref.at[grp, chunk],
            own_sem.at[chunk],
        )

    def stat_copy(step):
        return remote(
            stat_send.at[lax.rem(grp + step, groups)], stat_recv.at[grp], stat_sems, (step,), step
        )

    def square_copy(across, along):
        return remote(
            square_send.at[lax.rem(grp + across, groups)], square_recv.at[grp * rows + row],
            square_sems, (across, along), across, along,
        )

    def square_start(across, along, carry):
        square_copy(across, along).start()
        return carry

    def square_wait(across, along, carry):
        square_copy(across, along).wait()
        return carry

    column = grid_iota((wanted, LANES), 0) % wanted_dev

    def compute(chunk, carry):
        stats, sums = carry
        for copy in loads(chunk):
            copy.wait()
        both = jnp.concatenate(
            [fields[which, chunk].reshape(padded_len * TILE, inner_dev) for which in range(2)], axis=1
        )
        product = jnp.dot(expanded[...], both, preferred_element_type=jnp.float32)
        product = product.reshape(wanted, TILE, 2 * inner_dev)
        ritz = product[:, :, :inner_dev]
        resid = product[:, :, inner_dev:] - shift_values * ritz
        for kind, cols in enumerate((ritz, resid)):
            squares = jnp.sum(jnp.sum(cols * cols, axis=1), axis=1, keepdims=True)
            most = jnp.max(jnp.max(jnp.abs(cols), axis=1), axis=1, keepdims=True)
            most = jnp.maximum(most, LEAST)
            codes = jnp.exp(SLOPE * jnp.log(1.0 + jnp.abs(cols) * expand_rows(SPREAD / most, inner_dev)) - REACH)
            codes = jnp.where(cols < 0.0, -codes, codes)
            coded[chunk, :, kind * inner_dev : (kind + 1) * inner_dev] = codes.reshape(
                wanted * TILE, inner_dev
            ).astype(jnp.bfloat16)
            stats = jnp.where(lane_stats == 2 * chunk + kind, most, stats)
            sums = jnp.where(lane_stats == column + kind * wanted_dev, sums + squares, sums)

        @pl.when(chunk == chunks - 1)
        def _():
            square_send[...] = jnp.sum(sums.reshape(groups, wanted_dev, LANES), axis=1, keepdims=True)
            others(square_start)
            stat_send[...] = stats.reshape(groups, wanted_dev, LANES)
            for step in range(1, groups):
                stat_copy(step).start()

        for step in range(1, groups):
            data_copy(chunk, step).start()
        own_copy(chunk).start()
        return stats, sums

    nothing = jnp.zeros((wanted, LANES), jnp.float32)
    lax.fori_loop(0, chunks, compute, (nothing, nothing))

    for step in range(1, groups):
        stat_copy(step).wait()
    stat_recv[grp] = stat_send[grp]
    stats_ref[...] = stat_recv[...]
    others(square_wait)
    square_recv[grp * rows + row] = square_send[grp]
    total_ref[...] = jnp.sum(square_recv[...], axis=0)

    def finish(chunk, carry):
        for step in range(1, groups):
            data_copy(chunk, step).wait()
        own_copy(chunk).wait()
        return carry

    lax.fori_loop(0, chunks, finish, 0)


def finish_kernel(rows_total, coded_ref, stats_ref, total_ref, ritz_ref, resid_ref, norm_ref):
    groups, wanted_dev = stats_ref.shape[:2]
    several = coded_ref.shape[1]
    first = pl.program_id(0) * several
    inner_dev = coded_ref.shape[3] // 2
    lanes = grid_iota((wanted_dev, LANES), 1)
    columns = grid_iota((wanted_dev, LANES), 0)

    def pick(tile, lane):
        return jnp.sum(jnp.where(lanes == lane, tile, 0.0), axis=1, keepdims=True)

    total = jnp.broadcast_to(total_ref[...], (wanted_dev, LANES))
    ritz_squares = pick(total, columns) + 1.0
    resid_squares = pick(total, columns + wanted_dev)
    factor = jnp.sqrt(rows_total / ritz_squares)
    for source in range(groups):
        for part in range(several):
            for kind, out_ref in enumerate((ritz_ref, resid_ref)):
                scale = pick(stats_ref[source], 2 * (first + part) + kind) * (factor * (1.0 / SPREAD))
                codes = coded_ref[source, part, :, kind * inner_dev : (kind + 1) * inner_dev].astype(jnp.float32)
                size = jnp.exp((jnp.log(jnp.abs(codes)) + REACH) * (1.0 / SLOPE)) - 1.0
                size = jnp.where(codes < 0.0, -size, size)
                size = size.reshape(wanted_dev, TILE, inner_dev) * expand_rows(scale, inner_dev)
                out_ref[:, part * TILE : (part + 1) * TILE, source * inner_dev : (source + 1) * inner_dev] = size
    norms = jnp.broadcast_to(jnp.sqrt(resid_squares / ritz_squares), (wanted_dev, LANES))
    norm_ref[...] = jnp.sum(jnp.where(lanes == columns, norms, 0.0), axis=0)[:wanted_dev]


def body(groups, rows, krylov_basis, krylov_image, tridiag_vectors, ritz_values):
    krylov_len, outer_dev, inner_dev = krylov_basis.shape
    wanted_dev = tridiag_vectors.shape[1]
    wanted = groups * wanted_dev
    chunks = outer_dev // TILE
    block = wanted_dev * TILE
    padded_len = cdiv(krylov_len, STEP) * STEP
    packed_width = cdiv(padded_len + 1, LANES) * LANES
    rows_total = float(outer_dev * inner_dev * groups * rows)
    f32, bf16 = jnp.float32, jnp.bfloat16
    dma = pltpu.SemaphoreType.DMA
    anywhere = pl.BlockSpec(memory_space=pl.ANY)
    vmem = pl.BlockSpec(memory_space=pltpu.VMEM)
    hbm = pl.BlockSpec(memory_space=pltpu.HBM)
    parts = cdiv(padded_len, LANES)
    several = 2 if chunks % 2 == 0 else 1
    coded, stats, total = pl.pallas_call(
        functools.partial(exchange_kernel, groups, rows, krylov_len),
        name="exchange",
        out_shape=(
            jax.ShapeDtypeStruct((groups, chunks, block, 2 * inner_dev), bf16),
            jax.ShapeDtypeStruct((groups, wanted_dev, LANES), f32),
            jax.ShapeDtypeStruct((1, LANES), f32),
        ),
        in_specs=[vmem, vmem, hbm, hbm],
        out_specs=(anywhere, vmem, vmem),
        scratch_shapes=[
            pltpu.VMEM((wanted_dev, packed_width), f32),
            pltpu.VMEM((groups, wanted_dev, packed_width), f32),
            pltpu.VMEM((2, chunks, padded_len, TILE, inner_dev), bf16),
            pltpu.VMEM((LANES, LANES * TILE), bf16),
            pltpu.VMEM((parts, wanted, LANES * TILE), f32),
            pltpu.VMEM((wanted * TILE, padded_len * TILE), bf16),
            pltpu.VMEM((chunks, wanted * TILE, 2 * inner_dev), bf16),
            pltpu.VMEM((groups, wanted_dev, LANES), f32),
            pltpu.VMEM((groups, wanted_dev, LANES), f32),
            pltpu.VMEM((groups, 1, LANES), f32),
            pltpu.VMEM((groups * rows, 1, LANES), f32),
            dma((2, chunks)),
            dma((2, groups)),
            dma((2, chunks, groups)),
            dma((chunks,)),
            dma((2, groups)),
            dma((2, groups, rows)),
        ],
        compiler_params=pltpu.CompilerParams(
            collective_id=0, has_side_effects=True, vmem_limit_bytes=52 * MIB
        ),
    )(tridiag_vectors.T, ritz_values[None], krylov_basis, krylov_image)
    ritz_vectors, ritz_residuals, norms = pl.pallas_call(
        functools.partial(finish_kernel, rows_total),
        name="finish",
        grid=(chunks // several,),
        out_shape=(
            jax.ShapeDtypeStruct((wanted_dev, outer_dev, groups * inner_dev), f32),
            jax.ShapeDtypeStruct((wanted_dev, outer_dev, groups * inner_dev), f32),
            jax.ShapeDtypeStruct((wanted_dev,), f32),
        ),
        in_specs=[
            pl.BlockSpec((groups, several, block, 2 * inner_dev), lambda c: (0, c, 0, 0)),
            pl.BlockSpec((groups, wanted_dev, LANES), lambda c: (0, 0, 0)),
            pl.BlockSpec((1, LANES), lambda c: (0, 0)),
        ],
        out_specs=(
            pl.BlockSpec((wanted_dev, several * TILE, groups * inner_dev), lambda c: (0, c, 0)),
            pl.BlockSpec((wanted_dev, several * TILE, groups * inner_dev), lambda c: (0, c, 0)),
            pl.BlockSpec((wanted_dev,), lambda c: (0,)),
        ),
        compiler_params=pltpu.CompilerParams(vmem_limit_bytes=16 * MIB),
    )(coded, stats, total)
    return ritz_vectors, ritz_residuals, norms


def solution(mesh):
    placed = (P(None, "row", "grp"), P(None, "row", "grp"), P(None, "grp"), P("grp"))
    return jax.shard_map(
        functools.partial(body, mesh.shape["grp"], mesh.shape["row"]),
        mesh=mesh,
        in_specs=placed,
        out_specs=(P("grp", "row", None), P("grp", "row", None), P("grp")),
        check_vma=False,
    )
```

```python
import functools
import math

import jax
import jax.numpy as jnp
from jax import lax
from jax.experimental import pallas as pl
from jax.experimental.pallas import tpu as pltpu
from jax.sharding import PartitionSpec as P

MESH = pl.DeviceIdType.MESH
MIB = 1 << 20
TILE = 8
STEP = 16
LANES = 128
SPREAD = 256.0
REACH = 86.0
SLOPE = 2.0 * REACH / math.log(1.0 + SPREAD)
LEAST = 1e-35


def cdiv(a, b):
    return (a + b - 1) // b


def grid_iota(shape, dim):
    return lax.broadcasted_iota(jnp.int32, shape, dim)


def expand_rows(cols, width):
    return jnp.broadcast_to(cols, (cols.shape[0], width)).reshape(cols.shape[0], 1, width)


def exchange_kernel(
    groups, rows, krylov_len,
    tridiag_ref, values_ref, basis_ref, image_ref,
    coded_ref, stats_ref, total_ref,
    packed_ref, coefs, fields, spread, reps, expanded, coded, stat_send, stat_recv, square_send, square_recv,
    load_sem, coef_sems, data_sems, own_sem, stat_sems, square_sems,
):
    wanted_dev, packed_width = packed_ref.shape
    wanted = groups * wanted_dev
    chunks = fields.shape[1]
    inner_dev = basis_ref.shape[2]
    padded_len = fields.shape[2]
    steps = padded_len // STEP
    wide = STEP * TILE
    block = wanted_dev * TILE
    grp = lax.axis_index("grp")
    row = lax.axis_index("row")
    lane_stats = grid_iota((wanted, LANES), 1)

    def loads(chunk):
        span = pl.ds(pl.multiple_of(chunk * TILE, TILE), TILE)
        return [
            pltpu.make_async_copy(
                ref.at[:, span, :], fields.at[which, chunk, pl.ds(0, krylov_len)], load_sem.at[which, chunk]
            )
            for which, ref in enumerate((basis_ref, image_ref))
        ]

    for chunk in range(chunks):
        for copy in loads(chunk):
            copy.start()

    near = grid_iota((wanted_dev, wanted_dev), 0) == grid_iota((wanted_dev, wanted_dev), 1)
    own_values = jnp.broadcast_to(values_ref[...].astype(jnp.float32), (wanted_dev, wanted_dev))
    own_values = jnp.sum(jnp.where(near, own_values, 0.0), axis=1, keepdims=True)
    packed_ref[...] = jnp.broadcast_to(own_values, (wanted_dev, packed_width))
    packed_ref[:, :krylov_len] = tridiag_ref[...].astype(jnp.float32)

    barrier = pltpu.get_barrier_semaphore()
    def others(action):
        for across in range(groups):
            lax.fori_loop(1 if across == 0 else 0, rows, functools.partial(action, across), 0)

    def device(across, along):
        return {"grp": lax.rem(grp + across, groups), "row": lax.rem(row + along, rows)}

    def greet(across, along, carry):
        pl.semaphore_signal(barrier, inc=1, device_id=device(across, along), device_id_type=MESH)
        return carry

    others(greet)
    pl.semaphore_wait(barrier, groups * rows - 1)

    def remote(src, dst, sems, index, across, along=0):
        return pltpu.make_async_remote_copy(
            src_ref=src,
            dst_ref=dst,
            send_sem=sems.at[(0,) + index],
            recv_sem=sems.at[(1,) + index],
            device_id=device(across, along),
            device_id_type=MESH,
        )

    def coef_copy(step):
        return remote(packed_ref, coefs.at[grp], coef_sems, (step,), step)

    for step in range(1, groups):
        coef_copy(step).start()
    coefs[grp] = packed_ref[...]

    if padded_len > krylov_len:
        for chunk in range(chunks):
            for which in range(2):
                fields[which, chunk, pl.ds(krylov_len, padded_len - krylov_len)] = jnp.zeros(
                    (padded_len - krylov_len, TILE, inner_dev), jnp.bfloat16
                )
    shape = spread.shape
    spread[...] = jnp.where(
        lax.shift_right_logical(grid_iota(shape, 1), 3) == grid_iota(shape, 0), 1.0, 0.0
    ).astype(jnp.bfloat16)

    for step in range(1, groups):
        coef_copy(step).wait()

    all_coefs = coefs[...].reshape(wanted, packed_width)
    shift_values = expand_rows(all_coefs[:, packed_width - 1 :], inner_dev)
    for part in range(cdiv(padded_len, LANES)):
        reps[part] = jnp.dot(
            all_coefs[:, part * LANES : (part + 1) * LANES].astype(jnp.bfloat16),
            spread[...],
            preferred_element_type=jnp.float32,
        )
    per_part = LANES // STEP
    same = (grid_iota((TILE, wide), 1) & (TILE - 1)) == grid_iota((TILE, wide), 0)
    for step in range(steps):
        at = (step % per_part) * wide
        values = reps[step // per_part, :, at : at + wide]
        values = jnp.where(same[None], values.reshape(wanted, 1, wide), 0.0)
        expanded[:, step * wide : (step + 1) * wide] = values.reshape(wanted * TILE, wide).astype(jnp.bfloat16)

    def data_copy(chunk, step):
        dest = lax.rem(grp + step, groups)
        return remote(
            coded.at[chunk, pl.ds(pl.multiple_of(dest * block, block), block)],
            coded_ref.at[grp, chunk],
            data_sems, (chunk, step), step,
        )

    def own_copy(chunk):
        return pltpu.make_async_copy(
            coded.at[chunk, pl.ds(pl.multiple_of(grp * block, block), block)],
            coded_ref.at[grp, chunk],
            own_sem.at[chunk],
        )

    def stat_copy(step):
        return remote(
            stat_send.at[lax.rem(grp + step, groups)], stat_recv.at[grp], stat_sems, (step,), step
        )

    def square_copy(across, along):
        return remote(
            square_send.at[lax.rem(grp + across, groups)], square_recv.at[grp * rows + row],
            square_sems, (across, along), across, along,
        )

    def square_start(across, along, carry):
        square_copy(across, along).start()
        return carry

    def square_wait(across, along, carry):
        square_copy(across, along).wait()
        return carry

    column = grid_iota((wanted, LANES), 0) % wanted_dev

    def compute(chunk, carry):
        stats, sums = carry
        for copy in loads(chunk):
            copy.wait()
        both = jnp.concatenate(
            [fields[which, chunk].reshape(padded_len * TILE, inner_dev) for which in range(2)], axis=1
        )
        product = jnp.dot(expanded[...], both, preferred_element_type=jnp.float32)
        product = product.reshape(wanted, TILE, 2 * inner_dev)
        ritz = product[:, :, :inner_dev]
        resid = product[:, :, inner_dev:] - shift_values * ritz
        for kind, cols in enumerate((ritz, resid)):
            squares = jnp.sum(jnp.sum(cols * cols, axis=1), axis=1, keepdims=True)
            most = jnp.max(jnp.max(jnp.abs(cols), axis=1), axis=1, keepdims=True)
            most = jnp.maximum(most, LEAST)
            codes = jnp.exp(SLOPE * jnp.log(1.0 + jnp.abs(cols) * expand_rows(SPREAD / most, inner_dev)) - REACH)
            codes = jnp.where(cols < 0.0, -codes, codes)
            coded[chunk, :, kind * inner_dev : (kind + 1) * inner_dev] = codes.reshape(
                wanted * TILE, inner_dev
            ).astype(jnp.bfloat16)
            stats = jnp.where(lane_stats == 2 * chunk + kind, most, stats)
            sums = jnp.where(lane_stats == column + kind * wanted_dev, sums + squares, sums)

        @pl.when(chunk == chunks - 1)
        def _():
            square_send[...] = jnp.sum(sums.reshape(groups, wanted_dev, LANES), axis=1, keepdims=True)
            others(square_start)
            stat_send[...] = stats.reshape(groups, wanted_dev, LANES)
            for step in range(1, groups):
                stat_copy(step).start()

        for step in range(1, groups):
            data_copy(chunk, step).start()
        own_copy(chunk).start()
        return stats, sums

    nothing = jnp.zeros((wanted, LANES), jnp.float32)
    lax.fori_loop(0, chunks, compute, (nothing, nothing))

    for step in range(1, groups):
        stat_copy(step).wait()
    stat_recv[grp] = stat_send[grp]
    stats_ref[...] = stat_recv[...]
    others(square_wait)
    square_recv[grp * rows + row] = square_send[grp]
    total_ref[...] = jnp.sum(square_recv[...], axis=0)

    def finish(chunk, carry):
        for step in range(1, groups):
            data_copy(chunk, step).wait()
        own_copy(chunk).wait()
        return carry

    lax.fori_loop(0, chunks, finish, 0)


def finish_kernel(rows_total, coded_ref, stats_ref, total_ref, ritz_ref, resid_ref, norm_ref):
    groups, wanted_dev = stats_ref.shape[:2]
    several = coded_ref.shape[1]
    first = pl.program_id(0) * several
    inner_dev = coded_ref.shape[3] // 2
    lanes = grid_iota((wanted_dev, LANES), 1)
    columns = grid_iota((wanted_dev, LANES), 0)

    def pick(tile, lane):
        return jnp.sum(jnp.where(lanes == lane, tile, 0.0), axis=1, keepdims=True)

    total = jnp.broadcast_to(total_ref[...], (wanted_dev, LANES))
    ritz_squares = pick(total, columns) + 1.0
    resid_squares = pick(total, columns + wanted_dev)
    factor = jnp.sqrt(rows_total / ritz_squares)
    for source in range(groups):
        for part in range(several):
            for kind, out_ref in enumerate((ritz_ref, resid_ref)):
                scale = pick(stats_ref[source], 2 * (first + part) + kind) * (factor * (1.0 / SPREAD))
                codes = coded_ref[source, part, :, kind * inner_dev : (kind + 1) * inner_dev].astype(jnp.float32)
                size = jnp.exp((jnp.log(jnp.abs(codes)) + REACH) * (1.0 / SLOPE)) - 1.0
                size = jnp.where(codes < 0.0, -size, size)
                size = size.reshape(wanted_dev, TILE, inner_dev) * expand_rows(scale, inner_dev)
                out_ref[:, part * TILE : (part + 1) * TILE, source * inner_dev : (source + 1) * inner_dev] = size
    norms = jnp.broadcast_to(jnp.sqrt(resid_squares / ritz_squares), (wanted_dev, LANES))
    norm_ref[...] = jnp.sum(jnp.where(lanes == columns, norms, 0.0), axis=0)[:wanted_dev]


def body(groups, rows, krylov_basis, krylov_image, tridiag_vectors, ritz_values):
    krylov_len, outer_dev, inner_dev = krylov_basis.shape
    wanted_dev = tridiag_vectors.shape[1]
    wanted = groups * wanted_dev
    chunks = outer_dev // TILE
    block = wanted_dev * TILE
    padded_len = cdiv(krylov_len, STEP) * STEP
    packed_width = cdiv(padded_len + 1, LANES) * LANES
    rows_total = float(outer_dev * inner_dev * groups * rows)
    f32, bf16 = jnp.float32, jnp.bfloat16
    dma = pltpu.SemaphoreType.DMA
    anywhere = pl.BlockSpec(memory_space=pl.ANY)
    vmem = pl.BlockSpec(memory_space=pltpu.VMEM)
    hbm = pl.BlockSpec(memory_space=pltpu.HBM)
    parts = cdiv(padded_len, LANES)
    several = math.gcd(chunks, 4)
    coded, stats, total = pl.pallas_call(
        functools.partial(exchange_kernel, groups, rows, krylov_len),
        name="exchange",
        out_shape=(
            jax.ShapeDtypeStruct((groups, chunks, block, 2 * inner_dev), bf16),
            jax.ShapeDtypeStruct((groups, wanted_dev, LANES), f32),
            jax.ShapeDtypeStruct((1, LANES), f32),
        ),
        in_specs=[vmem, vmem, hbm, hbm],
        out_specs=(anywhere, vmem, vmem),
        scratch_shapes=[
            pltpu.VMEM((wanted_dev, packed_width), f32),
            pltpu.VMEM((groups, wanted_dev, packed_width), f32),
            pltpu.VMEM((2, chunks, padded_len, TILE, inner_dev), bf16),
            pltpu.VMEM((LANES, LANES * TILE), bf16),
            pltpu.VMEM((parts, wanted, LANES * TILE), f32),
            pltpu.VMEM((wanted * TILE, padded_len * TILE), bf16),
            pltpu.VMEM((chunks, wanted * TILE, 2 * inner_dev), bf16),
            pltpu.VMEM((groups, wanted_dev, LANES), f32),
            pltpu.VMEM((groups, wanted_dev, LANES), f32),
            pltpu.VMEM((groups, 1, LANES), f32),
            pltpu.VMEM((groups * rows, 1, LANES), f32),
            dma((2, chunks)),
            dma((2, groups)),
            dma((2, chunks, groups)),
            dma((chunks,)),
            dma((2, groups)),
            dma((2, groups, rows)),
        ],
        compiler_params=pltpu.CompilerParams(
            collective_id=0, has_side_effects=True, vmem_limit_bytes=52 * MIB
        ),
    )(tridiag_vectors.T, ritz_values[None], krylov_basis, krylov_image)
    ritz_vectors, ritz_residuals, norms = pl.pallas_call(
        functools.partial(finish_kernel, rows_total),
        name="finish",
        grid=(chunks // several,),
        out_shape=(
            jax.ShapeDtypeStruct((wanted_dev, outer_dev, groups * inner_dev), f32),
            jax.ShapeDtypeStruct((wanted_dev, outer_dev, groups * inner_dev), f32),
            jax.ShapeDtypeStruct((wanted_dev,), f32),
        ),
        in_specs=[
            pl.BlockSpec((groups, several, block, 2 * inner_dev), lambda c: (0, c, 0, 0)),
            pl.BlockSpec((groups, wanted_dev, LANES), lambda c: (0, 0, 0)),
            pl.BlockSpec((1, LANES), lambda c: (0, 0)),
        ],
        out_specs=(
            pl.BlockSpec((wanted_dev, several * TILE, groups * inner_dev), lambda c: (0, c, 0)),
            pl.BlockSpec((wanted_dev, several * TILE, groups * inner_dev), lambda c: (0, c, 0)),
            pl.BlockSpec((wanted_dev,), lambda c: (0,)),
        ),
        compiler_params=pltpu.CompilerParams(vmem_limit_bytes=16 * MIB),
    )(coded, stats, total)
    return ritz_vectors, ritz_residuals, norms


def solution(mesh):
    placed = (P(None, "row", "grp"), P(None, "row", "grp"), P(None, "grp"), P("grp"))
    return jax.shard_map(
        functools.partial(body, mesh.shape["grp"], mesh.shape["row"]),
        mesh=mesh,
        in_specs=placed,
        out_specs=(P("grp", "row", None), P("grp", "row", None), P("grp")),
        check_vma=False,
    )
```
